128 devices in a mesh: doc: 8 (over z_lo, y), ctx: 16 (over x, z_hi, core).
Axes of the slice: x: 4, y: 4, z: 4 (z_hi: 2, z_lo: 2; z = z_hi * 2 + z_lo), core: 2. Of those that a mesh axis runs over, the one named last changes fastest.
Arguments:
- summary_cache: bfloat16 [8, 64, 512, 2048], P(None, 'doc', None, 'ctx'), may hold values from -4 to 4
- queries: bfloat16 [8, 4096, 4096], P('doc', 'ctx'), may hold values from -100 to 100
- section_counts: int32 [64], replicated, may hold values from 1 to 2
- summary_blocks: int32 [64, 2], replicated, may hold values from 1 to 2
Outputs:
- attended: bfloat16 [8, 4096, 4096], P('doc', 'ctx')
- relayed: bfloat16 [8, 8, 4096, 2048], P(None, 'doc', 'ctx')
The draws below stay inside these ranges and needn't reach their ends.
All inputs are finite; a program needn't handle non-finite values.
Results may differ from the reference program's by a relative error of at most 0.0045.
Values may be sent and summed in bfloat16 or wider, within the bound.
A program may use at most 192 MiB of HBM per device.

```python
import math
import jax
import jax.numpy as jnp
from jax import lax

QH = 32
KVH = 8
HD = 128
LAYERS = 8
BLOCK = 128
SUMBLK = 2
SECTIONS = 2
GROUP = 4
FEAT = 2048
SUMLEN = 256
SEQD = 512
GROUPS = 8
DOCS = 64
GSEQ = 4096


def draw_summary_cache(key, part):
    array_shape = (LAYERS, DOCS, SEQD, FEAT)
    base_key = jax.random.fold_in(key, 3)
    values = jnp.clip(jax.random.normal(base_key, array_shape, jnp.float32), -4.0, 4.0)
    return values.astype(jnp.bfloat16)


def draw_queries(key, part):
    array_shape = (GROUPS, GSEQ, QH * HD)
    base_key = jax.random.fold_in(key, 5)
    values = jnp.clip(jax.random.normal(base_key, array_shape, jnp.float32), -4.0, 4.0)
    return values.astype(jnp.bfloat16)


def with_ends(values, key, least, largest):
    longest = values.shape.index(max(values.shape))
    spots = []
    for shift in (0, 1):
        where = [jax.random.randint(jax.random.fold_in(key, axis), (), 0, length) for axis, length in enumerate(values.shape)]
        where[longest] = (where[longest] + shift) % values.shape[longest]
        spots.append(tuple(where))
    return values.at[spots[0]].set(least).at[spots[1]].set(largest)


def setup_inputs(seed: int = 0) -> dict:
    arg_keys = jax.random.split(jax.random.key(seed), 5)
    summary_cache = draw_summary_cache(jax.random.fold_in(arg_keys[4], 71), 0)
    queries = draw_queries(jax.random.fold_in(arg_keys[4], 71), 0)
    section_counts = with_ends(jax.random.randint(arg_keys[2], (DOCS,), 1, SECTIONS + 1), jax.random.fold_in(arg_keys[2], 1), 1, SECTIONS).astype(jnp.int32)
    summary_blocks = with_ends(jax.random.randint(arg_keys[3], (DOCS, SECTIONS), 1, SUMBLK + 1), jax.random.fold_in(arg_keys[3], 1), 1, SUMBLK).astype(jnp.int32)
    return dict(summary_cache=summary_cache, queries=queries, section_counts=section_counts, summary_blocks=summary_blocks)


NEGATIVE = -1e+30

def attend_group(operands):
    query_rows, key_rows, validity = operands
    block_rows = min(GSEQ, 512)
    pieces = []
    for offset in range(0, GSEQ, block_rows):
        key_end = offset + block_rows
        grouped = query_rows[offset:key_end].astype(jnp.float32).reshape(block_rows, KVH, GROUP, HD)
        key_heads = key_rows[:key_end, :KVH * HD].astype(jnp.float32).reshape(key_end, KVH, HD)
        value_heads = key_rows[:key_end, KVH * HD:].astype(jnp.float32).reshape(key_end, KVH, HD)
        scores = jnp.einsum('pkgd,skd->kgps', grouped, key_heads) * (1.0 / math.sqrt(HD))
        key_positions = jnp.arange(key_end)
        query_positions = offset + jnp.arange(block_rows)
        allowed = validity[None, :key_end] & (key_positions[None, :] <= query_positions[:, None])
        masked = jnp.where(allowed, scores, NEGATIVE)
        row_maximum = lax.optimization_barrier(jnp.max(masked, axis=-1, keepdims=True))
        weights = jnp.where(allowed, jnp.exp(masked - row_maximum), 0.0)
        denominator = lax.optimization_barrier(jnp.sum(weights, axis=-1))
        rounded = lax.optimization_barrier(weights.astype(jnp.bfloat16)).astype(jnp.float32)
        accumulated = jnp.einsum('kgps,skd->kgpd', rounded, value_heads)
        result = accumulated / denominator[..., None]
        pieces.append(jnp.transpose(result, (2, 0, 1, 3)).reshape(block_rows, QH * HD))
    return jnp.concatenate(pieces, axis=0).astype(jnp.bfloat16)

def reference(summary_cache, queries, section_counts, summary_blocks):
    relayed = jnp.transpose(summary_cache.reshape(LAYERS, GROUPS, GROUPS, SEQD, FEAT), (0, 2, 1, 3, 4)).reshape(LAYERS, GROUPS, GSEQ, FEAT)
    counts_table = jnp.transpose(section_counts.reshape(GROUPS, GROUPS), (1, 0))
    blocks_table = jnp.transpose(summary_blocks.reshape(GROUPS, GROUPS, SECTIONS), (1, 0, 2))
    live_section = jnp.arange(SECTIONS)[None, None, :] < counts_table[:, :, None]
    live_slot = jnp.arange(SUMLEN)[None, None, None, :] < BLOCK * blocks_table[:, :, :, None]
    validity = (live_section[..., None] & live_slot).reshape(GROUPS, GSEQ)
    attended = lax.map(attend_group, (queries, relayed[0], validity))
    return (attended, relayed)
```

```python
import functools
import math

import jax
import jax.numpy as jnp
from jax import lax
from jax.experimental import pallas as pl
from jax.experimental.pallas import tpu as pltpu
from jax.sharding import PartitionSpec as P

HD = 128
BLOCK = 128
SECTIONS = 2
GROUP = 4
SUMLEN = 256
XS = 4

NEGATIVE = -1e30
MESH = pl.DeviceIdType.MESH


def mult(v, n):
    return pl.multiple_of(v * n, n)


def kernel(
    rows,
    ctx,
    cache,
    queries,
    counts,
    blocks,
    attended,
    relayed,
    kv,
    mid,
    q_in,
    out_v,
    live,
    causal,
    kv_sem,
    q_sem,
    r1,
    r2,
    r0,
    ro,
    s_kv,
    s_fwd,
    s_q,
    s1,
    s2,
    s0,
    so,
):
    layers, _, slots, feat = cache.shape
    own = queries.shape[0]
    wide = GROUP * HD
    me = lax.axis_index("doc")
    c = lax.axis_index("ctx")
    x = c // 4
    zh = (c // 2) % 2
    core = c % 2

    def at(xx, z, o):
        return 4 * xx + 2 * z + o

    barrier = pltpu.get_barrier_semaphore()
    greeted = 0
    for k in range(rows):
        for dx in range(XS):
            for n in range(4):
                if (k, dx, n) == (0, 0, 0) or (k > 0 and dx % 2 == 1):
                    continue
                greeted += 1
                pl.semaphore_signal(
                    barrier,
                    inc=1,
                    device_id=((me + k) % rows, 4 * ((x + dx) % XS) + (c + n) % 4),
                    device_id_type=MESH,
                )

    kind = x // 2
    owner = at(x % 2 + 2 * core, zh, zh)
    head = 4 * (x % 2) + 2 * core + x // 2

    def remote(src, dst, send, recv, row, target):
        return pltpu.make_async_remote_copy(
            src_ref=src,
            dst_ref=dst,
            send_sem=send,
            recv_sem=recv,
            device_id=(row, target),
            device_id_type=MESH,
        )

    def sized(ref, sem):
        return pltpu.make_async_copy(ref, ref, sem)

    def doc(which, j):
        return kv.at[which, pl.ds(mult(j, slots), slots)]

    pl.semaphore_wait(barrier, greeted)

    @pl.when(owner != c)
    def _():
        remote(cache.at[0, me], doc(kind, me), s_kv, kv_sem.at[kind, me], me, owner).start()

    @pl.when(owner == c)
    def _():
        pltpu.make_async_copy(cache.at[0, me], doc(kind, me), kv_sem.at[kind, me]).start()

    for k in range(1, rows):
        g = (me + k) % rows
        remote(cache.at[0, g], doc(kind, me), s_kv, kv_sem.at[kind, me], g, owner).start()

    q_to = q_in.at[pl.ds(pl.multiple_of(512 * x + own * core, own), own)]
    for dx in (2, 1, 3, 0):
        for do in range(2):
            xx = (x + dx) % XS
            oo = (core + do) % 2
            k = 4 * (xx % 2) + 2 * oo + xx // 2
            src = queries.at[:, pl.ds(mult(k, wide), wide)]
            if dx == 0 and do == 0:
                pltpu.make_async_copy(src, q_to, q_sem.at[x]).start()
            else:
                remote(src, q_to, s_q, q_sem.at[x], me, at(xx, zh, oo)).start()

    def gather(l):
        dst = mid.at[l - 1, me // 2, :, pl.ds(mult(2 * zh + core, feat), feat)]
        for k in range(rows):
            g = (me + k) % rows
            for n in range(2):
                h = (core + n) % 2
                src = cache.at[l, g, pl.ds(mult(h, own), own)]
                copy = remote(src, dst, s1, r1.at[l], g, at(x, me % 2, h))
                if k == 0 and n == 0:

                    @pl.when(zh != me % 2)
                    def _():
                        copy.start()

                    @pl.when(zh == me % 2)
                    def _():
                        pltpu.make_async_copy(src, dst, r1.at[l]).start()
                else:
                    copy.start()

    def spread(l):
        sized(mid.at[l - 1], r1.at[l]).wait()
        dst = relayed.at[l, :, pl.ds(mult(x, wide), wide)]
        for dx in (2, 1, 3, 0):
            xx = (x + dx) % XS
            if dx:
                remote(mid.at[l - 1, xx], dst, s2, r2, me, at(xx, zh, core)).start()
            else:
                pltpu.make_async_copy(mid.at[l - 1, xx], dst, r2).start()

    @pl.loop(1, layers)
    def _(l):
        gather(l)

    key = lax.broadcasted_iota(jnp.int32, (8, slots), 1)

    @pl.loop(0, rows)
    def _(j):
        document = j * rows + me
        section = key // SUMLEN
        reach = jnp.zeros((8, slots), jnp.int32)
        for s in range(SECTIONS):
            reach = jnp.where(
                (section == s) & (s < counts[document]), BLOCK * blocks[document, s], reach
            )
        live[j] = jnp.where(key - section * SUMLEN < reach, 0.0, NEGATIVE)

    @pl.loop(0, slots // 8)
    def _(r):
        query = lax.broadcasted_iota(jnp.int32, (8, slots), 0) + 8 * r
        causal[pl.ds(mult(r, 8), 8)] = jnp.where(key <= query, 0.0, NEGATIVE)

    for k in range(rows):
        j = (me + k) % rows
        for which in range(2):
            block = doc(which, j)
            sized(block, kv_sem.at[which, j]).wait()

            @pl.when(zh == core)
            def _():
                remote(block, block, s_fwd, kv_sem.at[which, j], me, at(x, 1 - zh, core)).start()

    for which in range(2):
        for dx in (2, 1, 3, 0):
            for do in range(2):
                t = at((x + dx) % XS, zh, (core + do) % 2)
                src = kv.at[which, pl.ds(mult(t, own), own)]
                dst = relayed.at[0, :, pl.ds(pl.multiple_of(1024 * which + HD * head, HD), HD)]
                if dx == 0 and do == 0:
                    pltpu.make_async_copy(src, dst, r0).start()
                else:
                    remote(src, dst, s0, r0, me, t).start()

    factor = math.log2(math.e) / math.sqrt(HD)
    to = attended.at[:, pl.ds(mult(head, wide), wide)]

    for step, dx in enumerate((2, 1, 3, 0)):
        xt = (x + dx) % XS
        m = 2 * xt + zh
        row = pl.ds(mult(xt, slots), slots)
        sized(q_in.at[row], q_sem.at[xt]).wait()

        @pl.loop(0, GROUP)
        def _(i):
            l = 1 + 2 * step + i // 2

            @pl.when((i % 2 == 0) & (l < layers))
            def _():
                spread(l)

            column = pl.ds(mult(i, HD), HD)
            q = q_in[row, column]

            def block(j, state, bias):
                top, total, acc = state
                keys = pl.ds(mult(j, slots), slots)
                s = lax.dot_general(
                    q, kv[0, keys], (((1,), (1,)), ((), ())), preferred_element_type=jnp.float32
                )
                s = s + bias
                newest = jnp.maximum(top, jnp.max(s, axis=1, keepdims=True))
                w = jnp.exp2((s - newest) * factor)
                shrink = jnp.exp2((top - newest) * factor)
                total = total * shrink + jnp.sum(w, axis=1, keepdims=True)
                acc = acc * shrink + jnp.dot(
                    w.astype(jnp.bfloat16), kv[1, keys], preferred_element_type=jnp.float32
                )
                return newest, total, acc

            state = (
                jnp.full((slots, 1), NEGATIVE, jnp.float32),
                jnp.zeros((slots, 1), jnp.float32),
                jnp.zeros((slots, HD), jnp.float32),
            )
            state = lax.fori_loop(0, m, lambda j, st: block(j, st, live[j, 0:1]), state)
            _, total, acc = block(m, state, live[m, 0:1] + causal[...])
            out_v[row, column] = (acc / total).astype(jnp.bfloat16)

        for do in range(2):
            oo = (core + do) % 2
            src = out_v.at[pl.ds(pl.multiple_of(512 * xt + own * oo, own), own)]
            if dx == 0 and do == 0:
                pltpu.make_async_copy(src, to, ro).start()
            else:
                remote(src, to, so, ro, me, at(xt, zh, oo)).start()

    @pl.when(owner != c)
    def _():
        sized(cache.at[0, pl.ds(0, rows)], s_kv).wait()

    @pl.when(owner == c)
    def _():
        sized(cache.at[0, pl.ds(0, rows - 1)], s_kv).wait()

    @pl.when(zh == core)
    def _():
        sized(kv, s_fwd).wait()

    sized(q_in.at[pl.ds(0, 7 * own)], s_q).wait()

    @pl.when(zh != me % 2)
    def _():
        sized(cache.at[pl.ds(1, layers - 1)], s1).wait()

    @pl.when(zh == me % 2)
    def _():
        sized(cache.at[pl.ds(1, layers - 1), :, pl.ds(0, slots - slots // 16)], s1).wait()

    sized(mid.at[:, pl.ds(0, XS - 1)], s2).wait()
    sized(kv.at[:, pl.ds(0, 7 * own)], s0).wait()
    sized(out_v.at[pl.ds(0, 7 * own)], so).wait()
    sized(relayed.at[pl.ds(1, layers - 1)], r2).wait()
    sized(relayed.at[0], r0).wait()
    sized(attended, ro).wait()


def local(summary_cache, queries, section_counts, summary_blocks):
    rows = lax.axis_size("doc")
    ctx = lax.axis_size("ctx")
    layers, documents, slots, feat = summary_cache.shape
    own = queries.shape[1]
    wide = GROUP * HD
    dtype = summary_cache.dtype
    any_space = pl.BlockSpec(memory_space=pl.ANY)
    scalars = pl.BlockSpec(memory_space=pltpu.SMEM)
    dma = pltpu.SemaphoreType.DMA
    attended, relayed = pl.pallas_call(
        functools.partial(kernel, rows, ctx),
        out_shape=(
            jax.ShapeDtypeStruct(queries.shape[1:], dtype),
            jax.ShapeDtypeStruct((layers, own, ctx * feat), dtype),
        ),
        in_specs=[any_space, any_space, scalars, scalars],
        out_specs=(any_space, any_space),
        scratch_shapes=[
            pltpu.VMEM((2, rows * slots, feat), dtype),
            pltpu.VMEM((layers - 1, XS, own, wide), dtype),
            pltpu.VMEM((8 * own, wide), dtype),
            pltpu.VMEM((8 * own, wide), dtype),
            pltpu.VMEM((rows, 8, slots), jnp.float32),
            pltpu.VMEM((slots, slots), jnp.float32),
            dma((2, rows)),
            dma((XS,)),
            dma((layers,)),
            dma,
            dma,
            dma,
            dma,
            dma,
            dma,
            dma,
            dma,
            dma,
            dma,
        ],
        compiler_params=pltpu.CompilerParams(
            collective_id=0, has_side_effects=True, vmem_limit_bytes=60 * 1024 * 1024
        ),
    )(summary_cache, queries[0], section_counts, summary_blocks)
    return attended[None], relayed[:, None]


def solution(mesh):
    placed = (P(None, "doc", None, "ctx"), P("doc", "ctx", None), P(), P())
    return jax.shard_map(
        local,
        mesh=mesh,
        in_specs=placed,
        out_specs=(P("doc", "ctx", None), P(None, "doc", "ctx", None)),
        check_vma=False,
    )
```

```python
import functools
import math

import jax
import jax.numpy as jnp
from jax import lax
from jax.experimental import pallas as pl
from jax.experimental.pallas import tpu as pltpu
from jax.sharding import PartitionSpec as P

HD = 128
BLOCK = 128
SECTIONS = 2
GROUP = 4
SUMLEN = 256
XS = 4

NEGATIVE = -1e30
MESH = pl.DeviceIdType.MESH


def mult(v, n):
    return pl.multiple_of(v * n, n)


def kernel(
    rows,
    ctx,
    cache,
    queries,
    counts,
    blocks,
    attended,
    relayed,
    kv,
    mid,
    q_in,
    out_v,
    live,
    causal,
    kv_sem,
    q_sem,
    r1,
    r2,
    r0,
    ro,
    s_kv,
    s_fwd,
    s_q,
    s1,
    s2,
    s0,
    so,
):
    layers, _, slots, feat = cache.shape
    own = queries.shape[0]
    wide = GROUP * HD
    me = lax.axis_index("doc")
    c = lax.axis_index("ctx")
    x = c // 4
    zh = (c // 2) % 2
    core = c % 2

    def at(xx, z, o):
        return 4 * xx + 2 * z + o

    barrier = pltpu.get_barrier_semaphore()
    greeted = 0
    for k in range(rows):
        for dx in range(XS):
            for n in range(4):
                if (k, dx, n) == (0, 0, 0) or (k > 0 and dx % 2 == 1):
                    continue
                greeted += 1
                pl.semaphore_signal(
                    barrier,
                    inc=1,
                    device_id=((me + k) % rows, 4 * ((x + dx) % XS) + (c + n) % 4),
                    device_id_type=MESH,
                )

    kind = x // 2
    owner = at(x % 2 + 2 * core, zh, zh)
    head = 4 * (x % 2) + 2 * core + x // 2

    def remote(src, dst, send, recv, row, target):
        return pltpu.make_async_remote_copy(
            src_ref=src,
            dst_ref=dst,
            send_sem=send,
            recv_sem=recv,
            device_id=(row, target),
            device_id_type=MESH,
        )

    def sized(ref, sem):
        return pltpu.make_async_copy(ref, ref, sem)

    def doc(which, j):
        return kv.at[which, pl.ds(mult(j, slots), slots)]

    pl.semaphore_wait(barrier, greeted)

    @pl.when(owner != c)
    def _():
        remote(cache.at[0, me], doc(kind, me), s_kv, kv_sem.at[kind, me], me, owner).start()

    @pl.when(owner == c)
    def _():
        pltpu.make_async_copy(cache.at[0, me], doc(kind, me), kv_sem.at[kind, me]).start()

    for k in range(1, rows):
        g = (me + k) % rows
        remote(cache.at[0, g], doc(kind, me), s_kv, kv_sem.at[kind, me], g, owner).start()

    q_to = q_in.at[pl.ds(pl.multiple_of(512 * x + own * core, own), own)]
    for dx in (2, 1, 3, 0):
        for do in range(2):
            xx = (x + dx) % XS
            oo = (core + do) % 2
            k = 4 * (xx % 2) + 2 * oo + xx // 2
            src = queries.at[:, pl.ds(mult(k, wide), wide)]
            if dx == 0 and do == 0:
                pltpu.make_async_copy(src, q_to, q_sem.at[x]).start()
            else:
                remote(src, q_to, s_q, q_sem.at[x], me, at(xx, zh, oo)).start()

    def gather(l):
        dst = mid.at[l - 1, me // 2, :, pl.ds(mult(2 * zh + core, feat), feat)]
        for n in range(2):
            h = (core + n) % 2
            for k in (1, 7, 2, 6, 3, 5, 4, 0):
                g = (me + k) % rows
                src = cache.at[l, g, pl.ds(mult(h, own), own)]
                copy = remote(src, dst, s1, r1.at[l], g, at(x, me % 2, h))
                if k == 0 and n == 0:

                    @pl.when(zh != me % 2)
                    def _():
                        copy.start()

                    @pl.when(zh == me % 2)
                    def _():
                        pltpu.make_async_copy(src, dst, r1.at[l]).start()
                else:
                    copy.start()

    def spread(l):
        sized(mid.at[l - 1], r1.at[l]).wait()
        dst = relayed.at[l, :, pl.ds(mult(x, wide), wide)]
        for dx in (2, 1, 3, 0):
            xx = (x + dx) % XS
            if dx:
                remote(mid.at[l - 1, xx], dst, s2, r2, me, at(xx, zh, core)).start()
            else:
                pltpu.make_async_copy(mid.at[l - 1, xx], dst, r2).start()

    gather(1)

    key = lax.broadcasted_iota(jnp.int32, (8, slots), 1)

    @pl.loop(0, rows)
    def _(j):
        document = j * rows + me
        section = key // SUMLEN
        reach = jnp.zeros((8, slots), jnp.int32)
        for s in range(SECTIONS):
            reach = jnp.where(
                (section == s) & (s < counts[document]), BLOCK * blocks[document, s], reach
            )
        live[j] = jnp.where(key - section * SUMLEN < reach, 0.0, NEGATIVE)

    @pl.loop(0, slots // 8)
    def _(r):
        query = lax.broadcasted_iota(jnp.int32, (8, slots), 0) + 8 * r
        causal[pl.ds(mult(r, 8), 8)] = jnp.where(key <= query, 0.0, NEGATIVE)

    def arrived(k, which):
        block = doc(which, (me + k) % rows)
        sized(block, kv_sem.at[which, (me + k) % rows]).wait()
        return block

    @pl.when(zh == core)
    def _():
        for k in (0, 7, 1, 6, 2, 5, 3, 4):
            for which in range(2):
                block = arrived(k, which)
                remote(
                    block, block, s_fwd, kv_sem.at[which, (me + k) % rows], me, at(x, 1 - zh, core)
                ).start()

    spread(1)

    @pl.when(zh == core)
    def _():
        sized(kv, s_fwd).wait()

    @pl.when(zh != core)
    def _():
        for k in range(rows):
            for which in range(2):
                arrived(k, which)

    gather(2)
    gather(3)
    gather(4)

    for which in range(2):
        for dx in (2, 1, 3, 0):
            for do in range(2):
                t = at((x + dx) % XS, zh, (core + do) % 2)
                src = kv.at[which, pl.ds(mult(t, own), own)]
                dst = relayed.at[0, :, pl.ds(pl.multiple_of(1024 * which + HD * head, HD), HD)]
                if dx == 0 and do == 0:
                    pltpu.make_async_copy(src, dst, r0).start()
                else:
                    remote(src, dst, s0, r0, me, t).start()

    factor = math.log2(math.e) / math.sqrt(HD)
    to = attended.at[:, pl.ds(mult(head, wide), wide)]

    for step, dx in enumerate((2, 1, 3, 0)):
        xt = (x + dx) % XS
        m = 2 * xt + zh
        row = pl.ds(mult(xt, slots), slots)
        sized(q_in.at[row], q_sem.at[xt]).wait()

        @pl.loop(0, GROUP)
        def _(i):
            slot = GROUP * step + i

            @pl.when(slot % 3 == 2)
            def _():
                spread(2 + slot // 3)

            @pl.when((slot % 3 == 2) & (slot < 9))
            def _():
                gather(5 + slot // 3)

            column = pl.ds(mult(i, HD), HD)
            q = q_in[row, column]

            def block(j, state, bias):
                top, total, acc = state
                keys = pl.ds(mult(j, slots), slots)
                s = lax.dot_general(
                    q, kv[0, keys], (((1,), (1,)), ((), ())), preferred_element_type=jnp.float32
                )
                s = s + bias
                newest = jnp.maximum(top, jnp.max(s, axis=1, keepdims=True))
                w = jnp.exp2((s - newest) * factor)
                shrink = jnp.exp2((top - newest) * factor)
                total = total * shrink + jnp.sum(w, axis=1, keepdims=True)
                acc = acc * shrink + jnp.dot(
                    w.astype(jnp.bfloat16), kv[1, keys], preferred_element_type=jnp.float32
                )
                return newest, total, acc

            state = (
                jnp.full((slots, 1), NEGATIVE, jnp.float32),
                jnp.zeros((slots, 1), jnp.float32),
                jnp.zeros((slots, HD), jnp.float32),
            )
            state = lax.fori_loop(0, m, lambda j, st: block(j, st, live[j, 0:1]), state)
            _, total, acc = block(m, state, live[m, 0:1] + causal[...])
            out_v[row, column] = (acc / total).astype(jnp.bfloat16)

        for do in range(2):
            oo = (core + do) % 2
            src = out_v.at[pl.ds(pl.multiple_of(512 * xt + own * oo, own), own)]
            if dx == 0 and do == 0:
                pltpu.make_async_copy(src, to, ro).start()
            else:
                remote(src, to, so, ro, me, at(xt, zh, oo)).start()

    spread(7)

    @pl.when(owner != c)
    def _():
        sized(cache.at[0, pl.ds(0, rows)], s_kv).wait()

    @pl.when(owner == c)
    def _():
        sized(cache.at[0, pl.ds(0, rows - 1)], s_kv).wait()

    sized(q_in.at[pl.ds(0, 7 * own)], s_q).wait()

    @pl.when(zh != me % 2)
    def _():
        sized(cache.at[pl.ds(1, layers - 1)], s1).wait()

    @pl.when(zh == me % 2)
    def _():
        sized(cache.at[pl.ds(1, layers - 1), :, pl.ds(0, slots - slots // 16)], s1).wait()

    sized(mid.at[:, pl.ds(0, XS - 1)], s2).wait()
    sized(kv.at[:, pl.ds(0, 7 * own)], s0).wait()
    sized(out_v.at[pl.ds(0, 7 * own)], so).wait()
    sized(relayed.at[pl.ds(1, layers - 1)], r2).wait()
    sized(relayed.at[0], r0).wait()
    sized(attended, ro).wait()


def local(summary_cache, queries, section_counts, summary_blocks):
    rows = lax.axis_size("doc")
    ctx = lax.axis_size("ctx")
    layers, documents, slots, feat = summary_cache.shape
    own = queries.shape[1]
    wide = GROUP * HD
    dtype = summary_cache.dtype
    any_space = pl.BlockSpec(memory_space=pl.ANY)
    scalars = pl.BlockSpec(memory_space=pltpu.SMEM)
    dma = pltpu.SemaphoreType.DMA
    attended, relayed = pl.pallas_call(
        functools.partial(kernel, rows, ctx),
        out_shape=(
            jax.ShapeDtypeStruct(queries.shape[1:], dtype),
            jax.ShapeDtypeStruct((layers, own, ctx * feat), dtype),
        ),
        in_specs=[any_space, any_space, scalars, scalars],
        out_specs=(any_space, any_space),
        scratch_shapes=[
            pltpu.VMEM((2, rows * slots, feat), dtype),
            pltpu.VMEM((layers - 1, XS, own, wide), dtype),
            pltpu.VMEM((8 * own, wide), dtype),
            pltpu.VMEM((8 * own, wide), dtype),
            pltpu.VMEM((rows, 8, slots), jnp.float32),
            pltpu.VMEM((slots, slots), jnp.float32),
            dma((2, rows)),
            dma((XS,)),
            dma((layers,)),
            dma,
            dma,
            dma,
            dma,
            dma,
            dma,
            dma,
            dma,
            dma,
            dma,
        ],
        compiler_params=pltpu.CompilerParams(
            collective_id=0, has_side_effects=True, vmem_limit_bytes=60 * 1024 * 1024
        ),
    )(summary_cache, queries[0], section_counts, summary_blocks)
    return attended[None], relayed[:, None]


def solution(mesh):
    placed = (P(None, "doc", None, "ctx"), P("doc", "ctx", None), P(), P())
    return jax.shard_map(
        local,
        mesh=mesh,
        in_specs=placed,
        out_specs=(P("doc", "ctx", None), P(None, "doc", "ctx", None)),
        check_vma=False,
    )
```

```python
import functools
import math

import jax
import jax.numpy as jnp
from jax import lax
from jax.experimental import pallas as pl
from jax.experimental.pallas import tpu as pltpu
from jax.sharding import PartitionSpec as P

HD = 128
BLOCK = 128
SECTIONS = 2
GROUP = 4
SUMLEN = 256
XS = 4
YS = 4
ROUTES = ((1, 1), (3, 0), (2, 1), (0, 1), (1, 0), (3, 1), (2, 0), (0, 0))
SPREADS = ((2, 4), (3, 8), (4, 12), (5, 15), (6, 18))

NEGATIVE = -1e30
MESH = pl.DeviceIdType.MESH


def mult(v, n):
    return pl.multiple_of(v * n, n)


def kernel(
    rows,
    ctx,
    cache,
    queries,
    counts,
    blocks,
    attended,
    relayed,
    kv,
    mid,
    q_in,
    out_v,
    live,
    causal,
    kv_sem,
    q_sem,
    r1,
    r2,
    r0,
    ro,
    s_kv,
    s_q,
    s1,
    s2,
    s0,
    so,
):
    layers, _, slots, feat = cache.shape
    own = queries.shape[0]
    wide = GROUP * HD
    me = lax.axis_index("doc")
    c = lax.axis_index("ctx")
    x = c // 4
    zh = (c // 2) % 2
    core = c % 2

    def at(xx, z, o):
        return 4 * xx + 2 * z + o

    barrier = pltpu.get_barrier_semaphore()
    greeted = 0

    def greet(row, target):
        pl.semaphore_signal(barrier, inc=1, device_id=(row, target), device_id_type=MESH)

    for k in range(rows):
        row = (me + k) % rows
        for dx in (0, 2):
            for n in range(4):
                if (k, dx, n) != (0, 0, 0):
                    greet(row, 4 * ((x + dx) % XS) + (c + n) % 4)
                    greeted += 1
    for dx in (1, 3):
        for o in range(2):
            greet(me, at((x + dx) % XS, zh, o))
            greeted += 1

    def row_at(dy, dz):
        return YS * ((me // YS + dz) % 2) + (me + dy) % YS

    def head_of(xx, z, o):
        return 4 * (xx % 2) + 2 * o + (xx // 2 + z) % 2

    kind = x // 2
    near = x % 2 + 2 * core
    owners = (at(near, 0, zh), at((near + 2) % XS, 1, zh))
    head = head_of(x, zh, core)
    places = (
        (x, 1 - zh, 1 - zh, zh),
        ((x + 1) % XS, zh, 2, 3),
        ((x + 3) % XS, zh, 3, 2),
        (x, zh, zh, zh),
    )

    def remote(src, dst, send, recv, row, target):
        return pltpu.make_async_remote_copy(
            src_ref=src,
            dst_ref=dst,
            send_sem=send,
            recv_sem=recv,
            device_id=(row, target),
            device_id_type=MESH,
        )

    def sized(ref, sem):
        return pltpu.make_async_copy(ref, ref, sem)

    def doc(which, j):
        return kv.at[which, pl.ds(mult(j, slots), slots)]

    key = lax.broadcasted_iota(jnp.int32, (8, slots), 1)

    @pl.loop(0, rows)
    def _(j):
        document = j * rows + me
        section = key // SUMLEN
        reach = jnp.zeros((8, slots), jnp.int32)
        for s in range(SECTIONS):
            reach = jnp.where(
                (section == s) & (s < counts[document]), BLOCK * blocks[s, document], reach
            )
        live[j] = jnp.where(key - section * SUMLEN < reach, 0.0, NEGATIVE)

    @pl.loop(0, slots // 8)
    def _(r):
        query = lax.broadcasted_iota(jnp.int32, (8, slots), 0) + 8 * r
        causal[pl.ds(mult(r, 8), 8)] = jnp.where(key <= query, 0.0, NEGATIVE)

    pl.semaphore_wait(barrier, greeted)

    def first(owner, j):
        return remote(cache.at[0, j], doc(kind, me), s_kv, kv_sem.at[kind, me], j, owner)

    for owner in owners:

        @pl.when(owner != c)
        def _():
            first(owner, me).start()

        @pl.when(owner == c)
        def _():
            pltpu.make_async_copy(cache.at[0, me], doc(kind, me), kv_sem.at[kind, me]).start()

    for dy, dz in ROUTES[:-1]:
        for owner in owners:
            first(owner, row_at(dy, dz)).start()

    def ask():
        for n, (xx, z, _, slot) in enumerate(places):
            for do in range(2):
                oo = (core + do) % 2
                src = queries.at[:, pl.ds(mult(head_of(xx, z, oo), wide), wide)]
                dst = q_in.at[pl.ds(pl.multiple_of(slots * slot + own * core, own), own)]
                if n == len(places) - 1 and do == 0:
                    pltpu.make_async_copy(src, dst, q_sem.at[slot]).start()
                else:
                    remote(src, dst, s_q, q_sem.at[slot], me, at(xx, z, oo)).start()

    def gather(l):
        dst = mid.at[l - 1, me // 2, :, pl.ds(mult(2 * zh + core, feat), feat)]
        for n in range(2):
            h = (core + n) % 2
            for dy, dz in ROUTES:
                g = row_at(dy, dz)
                src = cache.at[l, g, pl.ds(mult(h, own), own)]
                copy = remote(src, dst, s1, r1.at[l], g, at(x, me % 2, h))
                if (dy, dz, n) == (0, 0, 0):

                    @pl.when(zh != me % 2)
                    def _():
                        copy.start()

                    @pl.when(zh == me % 2)
                    def _():
                        pltpu.make_async_copy(src, dst, r1.at[l]).start()
                else:
                    copy.start()

    def spread(l):
        sized(mid.at[l - 1], r1.at[l]).wait()
        dst = relayed.at[l, :, pl.ds(mult(x, wide), wide)]
        for dx in (2, 1, 3, 0):
            xx = (x + dx) % XS
            if dx:
                remote(mid.at[l - 1, xx], dst, s2, r2, me, at(xx, zh, core)).start()
            else:
                pltpu.make_async_copy(mid.at[l - 1, xx], dst, r2).start()

    ask()

    for which in range(2):
        for j in range(rows):
            sized(doc(which, j), kv_sem.at[which, j]).wait()

    for slot in range(XS):
        sized(q_in.at[pl.ds(slots * slot, slots)], q_sem.at[slot]).wait()

    @pl.loop(1, layers)
    def _(l):
        gather(l)

    for which in range(2):
        lanes = pl.ds(pl.multiple_of(1024 * which + HD * head, HD), HD)
        for n, (xx, z, _, _) in enumerate(places):
            for do in range(2):
                t = at(xx, z, (core + do) % 2)
                src = kv.at[which, pl.ds(mult(t, own), own)]
                dst = relayed.at[0, :, lanes]
                if n == len(places) - 1 and do == 0:
                    pltpu.make_async_copy(src, dst, r0).start()
                else:
                    remote(src, dst, s0, r0, me, t).start()

    spread(1)
    factor = math.log2(math.e) / math.sqrt(HD)
    to = attended.at[:, pl.ds(mult(head, wide), wide)]

    done = 0
    for n, (xt, zt, slot, _) in enumerate(places):
        m = 2 * xt + zt
        row = pl.ds(mult(slot, slots), slots)

        columns = [pl.ds(HD * i, HD) for i in range(GROUP)]

        def block(j, state, bias):
            keys = pl.ds(mult(j, slots), slots)
            shifted = []
            for column, (top, total, acc) in zip(columns, state):
                s = lax.dot_general(
                    q_in[row, column],
                    kv[0, keys],
                    (((1,), (1,)), ((), ())),
                    preferred_element_type=jnp.float32,
                )
                s = s + bias
                newest = jnp.maximum(top, jnp.max(s, axis=1, keepdims=True))
                w = jnp.exp2((s - newest) * factor)
                shrink = jnp.exp2((top - newest) * factor)
                total = total * shrink + jnp.sum(w, axis=1, keepdims=True)
                shifted.append((newest, total, acc * shrink, w.astype(jnp.bfloat16)))
            return tuple(
                (top, total, acc + jnp.dot(w, kv[1, keys], preferred_element_type=jnp.float32))
                for top, total, acc, w in shifted
            )

        def step_block(j, state):
            at_block = done + j
            for l, when in SPREADS:

                @pl.when(at_block == when)
                def _():
                    spread(l)

            return block(j, state, live[j, 0:1])

        state = (
            (
                jnp.full((slots, 1), NEGATIVE, jnp.float32),
                jnp.zeros((slots, 1), jnp.float32),
                jnp.zeros((slots, HD), jnp.float32),
            ),
        ) * GROUP
        state = lax.fori_loop(0, m, step_block, state)
        state = block(m, state, live[m, 0:1] + causal[...])
        for column, (_, total, acc) in zip(columns, state):
            out_v[row, column] = (acc / total).astype(jnp.bfloat16)
        done = done + m

        for do in range(2):
            oo = (core + do) % 2
            src = out_v.at[pl.ds(pl.multiple_of(slots * slot + own * oo, own), own)]
            if n == len(places) - 1 and do == 0:
                pltpu.make_async_copy(src, to, ro).start()
            else:
                remote(src, to, so, ro, me, at(xt, zt, oo)).start()

    for l, when in SPREADS:

        @pl.when(done <= when)
        def _():
            spread(l)

    for l in range(2 + len(SPREADS), layers):
        spread(l)

    @pl.when((kind == 0) & (zh == core))
    def _():
        sized(kv.at[:, pl.ds(0, (rows - 1) * slots + slots // 2)], s_kv).wait()

    @pl.when((kind == 1) | (zh != core))
    def _():
        sized(kv, s_kv).wait()

    sized(q_in.at[pl.ds(0, 7 * own)], s_q).wait()

    @pl.when(zh != me % 2)
    def _():
        sized(cache.at[pl.ds(1, layers - 1)], s1).wait()

    @pl.when(zh == me % 2)
    def _():
        sized(cache.at[pl.ds(1, layers - 1), :, pl.ds(0, slots - slots // 16)], s1).wait()

    sized(mid.at[:, pl.ds(0, XS - 1)], s2).wait()
    sized(kv.at[:, pl.ds(0, 7 * own)], s0).wait()
    sized(out_v.at[pl.ds(0, 7 * own)], so).wait()
    sized(relayed.at[pl.ds(1, layers - 1)], r2).wait()
    sized(relayed.at[0], r0).wait()
    sized(attended, ro).wait()


def place(attended, relayed, attended_out, relayed_out, sem):
    layers = relayed.shape[0]
    copies = [pltpu.make_async_copy(attended, attended_out, sem.at[layers])]
    copies += [pltpu.make_async_copy(relayed.at[l], relayed_out.at[l], sem.at[l]) for l in range(layers)]
    for copy in copies:
        copy.start()
    for copy in copies:
        copy.wait()


def local(summary_cache, queries, section_counts, summary_blocks):
    rows = lax.axis_size("doc")
    ctx = lax.axis_size("ctx")
    layers, documents, slots, feat = summary_cache.shape
    own = queries.shape[1]
    wide = GROUP * HD
    dtype = summary_cache.dtype
    any_space = pl.BlockSpec(memory_space=pl.ANY)
    hbm = pl.BlockSpec(memory_space=pltpu.MemorySpace.HBM)
    scalars = pl.BlockSpec(memory_space=pltpu.SMEM)
    dma = pltpu.SemaphoreType.DMA
    attended, relayed = pl.pallas_call(
        functools.partial(kernel, rows, ctx),
        out_shape=(
            pltpu.VMEM(queries.shape[1:], dtype),
            pltpu.VMEM((layers, own, ctx * feat), dtype),
        ),
        in_specs=[hbm, hbm, scalars, scalars],
        out_specs=(pl.BlockSpec(memory_space=pltpu.VMEM), pl.BlockSpec(memory_space=pltpu.VMEM)),
        scratch_shapes=[
            pltpu.VMEM((2, rows * slots, feat), dtype),
            pltpu.VMEM((layers - 1, XS, own, wide), dtype),
            pltpu.VMEM((8 * own, wide), dtype),
            pltpu.VMEM((8 * own, wide), dtype),
            pltpu.VMEM((rows, 8, slots), jnp.float32),
            pltpu.VMEM((slots, slots), jnp.float32),
            dma((2, rows)),
            dma((XS,)),
            dma((layers,)),
            dma,
            dma,
            dma,
            dma,
            dma,
            dma,
            dma,
            dma,
            dma,
        ],
        compiler_params=pltpu.CompilerParams(
            collective_id=0, has_side_effects=True, vmem_limit_bytes=52 * 1024 * 1024
        ),
    )(summary_cache, queries[0], section_counts, summary_blocks.T)
    vmem = pl.BlockSpec(memory_space=pltpu.VMEM)
    attended, relayed = pl.pallas_call(
        place,
        out_shape=(
            jax.ShapeDtypeStruct(attended.shape, dtype),
            jax.ShapeDtypeStruct(relayed.shape, dtype),
        ),
        in_specs=[vmem, vmem],
        out_specs=(any_space, any_space),
        scratch_shapes=[dma((layers + 1,))],
        compiler_params=pltpu.CompilerParams(vmem_limit_bytes=24 * 1024 * 1024),
    )(attended, relayed)
    return attended[None], relayed[:, None]


def solution(mesh):
    placed = (P(None, "doc", None, "ctx"), P("doc", "ctx", None), P(), P())
    return jax.shard_map(
        local,
        mesh=mesh,
        in_specs=placed,
        out_specs=(P("doc", "ctx", None), P(None, "doc", "ctx", None)),
        check_vma=False,
    )
```
